32 devices in a mesh: tile: 8 (over z, x), slab: 4 (over y, core).
Axes of the slice: x: 2, y: 2, z: 4, core: 2. Of those that a mesh axis runs over, the one named last changes fastest.
Arguments:
- object_field: float32 [2, 2, 4096, 2048], P(None, None, 'tile', 'slab')
- probe: float32 [2, 256, 256], replicated, may hold values from -5 to 5
- kernel_phase: float32 [256, 256], replicated, may hold values from -3.140625 to 3.140625
- measured: float32 [128, 256, 256], P(('tile', 'slab')), may hold values from 0.2 to 2
- positions: int32 [128, 2], P(('tile', 'slab')), may hold values from 0 to 3840, as said below
- batch: int32 [128], P(('tile', 'slab')), may hold values from 0 to 1
Outputs:
- object_new: float32 [2, 2, 4096, 2048], P(None, None, 'tile', 'slab')
- probe_new: float32 [2, 256, 256], replicated
The draws below stay inside these ranges and needn't reach their ends.
Inputs may be any that keep to these rules, and one draw needn't show every extreme that they name: `positions`: frame f's top-left pixel lies in the tile of rows t * 512 .. (t + 1) * 512 - 1 and columns s * 512 .. (s + 1) * 512 - 1, where t = (f // 4) // 4 and s = (f // 4) % 4; every frame lies inside the object.
All inputs are finite; a program needn't handle non-finite values.
Results may differ from the reference program's by a relative error of at most 0.0003.
Values sent between devices are 32-bit elements; how exact they have to be, the bound alone decides.
No kernel may reach another device: no remote copies, remote signals or barrier semaphores. Data moves between devices by JAX's collectives and lax.ppermute only.
A program may use at most 192 MiB of HBM per device.

```python
import math
import jax
import jax.numpy as jnp
from jax import lax

K = 256
LAYERS = 2
BATCHES = 2
TR = 512
TC = 512
F_DEV = 4
ROW_TILES = 8
COL_TILES = 4
NR = 4096
NC = 2048
FRAMES = 128


def draw_object_field(key, part):
    key_amp, key_phase = jax.random.split(jax.random.fold_in(key, 101))
    shape = (LAYERS, NR, NC)
    amplitude = jax.random.uniform(key_amp, shape, jnp.float32, 0.6, 1.2)
    phase = jax.random.uniform(key_phase, shape, jnp.float32, -math.pi, math.pi)
    return jnp.stack([amplitude * jnp.cos(phase), amplitude * jnp.sin(phase)], axis=0)


def draw_positions(key, part):
    key_row, key_col = jax.random.split(jax.random.fold_in(key, 202))
    frame = jnp.arange(FRAMES, dtype=jnp.int32)
    owner = frame // F_DEV
    row_tile = owner // COL_TILES
    col_tile = owner % COL_TILES
    row_top = jnp.where(row_tile == ROW_TILES - 1, TR - K + 1, TR).astype(jnp.int32)
    col_top = jnp.where(col_tile == COL_TILES - 1, TC - K + 1, TC).astype(jnp.int32)
    row_off = jax.random.randint(key_row, (FRAMES,), 0, row_top, dtype=jnp.int32)
    col_off = jax.random.randint(key_col, (FRAMES,), 0, col_top, dtype=jnp.int32)
    rows_at = row_tile * TR + row_off
    cols_at = col_tile * TC + col_off
    return jnp.stack([rows_at, cols_at], axis=1).astype(jnp.int32)


def plant(values, own_key, low, top_value):
    index_at = [jax.random.randint(jax.random.fold_in(own_key, axis), (), 0, length) for axis, length in enumerate(values.shape)]
    main_axis = values.shape.index(max(values.shape))
    next_to = index_at[:main_axis] + [(index_at[main_axis] + 1) % values.shape[main_axis]] + index_at[main_axis + 1:]
    return values.at[tuple(index_at)].set(low).at[tuple(next_to)].set(top_value)


def level_of(own_key, dims, cuts, least, largest):
    gain, own = 1.0, jax.random.fold_in(own_key, 6)
    for position, blocks in cuts:
        steps = jnp.exp(jax.random.uniform(jax.random.fold_in(own, position), (blocks,), jnp.float32, least / len(cuts), largest / len(cuts)))
        gain = gain * jnp.repeat(steps, dims[position] // blocks).reshape([-1 if axis == position else 1 for axis in range(len(dims))])
    return gain


def normal_values(own_key, dims, scale, bound, kind=jnp.bfloat16):
    entries = jax.random.normal(own_key, dims, jnp.float32) * scale
    return jnp.minimum(jnp.maximum(entries, -bound), bound).astype(kind)


def setup_inputs(seed: int = 0) -> dict:
    key_of = jax.random.split(jax.random.key(seed), 7)
    object_field = draw_object_field(jax.random.fold_in(key_of[6], 71), 0)
    probe = normal_values(key_of[1], (2, K, K), 0.7, 5.0, jnp.float32)
    kernel_phase = jnp.clip(jax.random.uniform(key_of[2], (K, K), jnp.float32, -3.140625, 3.140625), -3.140625, 3.140625)
    measured = jnp.clip(0.2 + 1.8 * jax.random.uniform(key_of[3], (FRAMES, K, K), jnp.float32) ** level_of(key_of[3], (FRAMES, K, K), ((0, 32),), -0.2, 0.2), 0.2, 2.0)
    positions = draw_positions(jax.random.fold_in(key_of[6], 71), 0)
    batch = plant(jax.random.randint(key_of[5], (FRAMES,), 0, 2), jax.random.fold_in(key_of[5], 1), 0, 1).astype(jnp.int32)
    return {"object_field": object_field, "probe": probe, "kernel_phase": kernel_phase, "measured": measured, "positions": positions, "batch": batch}


def dft_tables(size):
    index = jnp.arange(size, dtype=jnp.int32)
    product = index[:, None] * index[None, :] % size
    angles = product.astype(jnp.float32) * (2.0 * math.pi / size)
    norm_scale = 1.0 / math.sqrt(size)
    return (jnp.cos(angles) * norm_scale, -jnp.sin(angles) * norm_scale)

def matmul_pair(left_real, left_imag, right_real, right_imag):
    first = jnp.matmul(left_real, right_real, precision=lax.Precision.HIGHEST) - jnp.matmul(left_imag, right_imag, precision=lax.Precision.HIGHEST)
    second = jnp.matmul(left_real, right_imag, precision=lax.Precision.HIGHEST) + jnp.matmul(left_imag, right_real, precision=lax.Precision.HIGHEST)
    return (first, second)

def fourier(real_part, imag_part, cos_table, sin_table):
    mid_real, mid_imag = matmul_pair(real_part, imag_part, cos_table, sin_table)
    return matmul_pair(cos_table, sin_table, mid_real, mid_imag)

def frame_pass(patches, probe, kernel, measured, tables):
    cos_table, sin_table = tables
    back_sin = -sin_table
    kernel_real, kernel_imag = kernel
    patch_real = patches[:, 0]
    patch_imag = patches[:, 1]
    layers = patches.shape[2]
    wave_real = probe[0] * patch_real[:, 0] - probe[1] * patch_imag[:, 0]
    wave_imag = probe[0] * patch_imag[:, 0] + probe[1] * patch_real[:, 0]
    incoming = []
    for layer in range(1, layers):
        freq_real, freq_imag = fourier(wave_real, wave_imag, cos_table, sin_table)
        prop_real = freq_real * kernel_real - freq_imag * kernel_imag
        prop_imag = freq_real * kernel_imag + freq_imag * kernel_real
        in_real, in_imag = fourier(prop_real, prop_imag, cos_table, back_sin)
        incoming.append((in_real, in_imag))
        wave_real = patch_real[:, layer] * in_real - patch_imag[:, layer] * in_imag
        wave_imag = patch_real[:, layer] * in_imag + patch_imag[:, layer] * in_real
    far_real, far_imag = fourier(wave_real, wave_imag, cos_table, sin_table)
    power = far_real * far_real + far_imag * far_imag
    factor = 1.0 - measured / jnp.sqrt(jnp.maximum(power, 0.01))
    grad_real, grad_imag = fourier(far_real * factor, far_imag * factor, cos_table, back_sin)
    layer_grads = [None] * layers
    for layer in range(layers - 1, 0, -1):
        in_real, in_imag = incoming[layer - 1]
        layer_grads[layer] = (in_real * grad_real + in_imag * grad_imag, in_real * grad_imag - in_imag * grad_real)
        back_real = patch_real[:, layer] * grad_real + patch_imag[:, layer] * grad_imag
        back_imag = patch_real[:, layer] * grad_imag - patch_imag[:, layer] * grad_real
        freq_real, freq_imag = fourier(back_real, back_imag, cos_table, sin_table)
        conj_real = freq_real * kernel_real + freq_imag * kernel_imag
        conj_imag = freq_imag * kernel_real - freq_real * kernel_imag
        grad_real, grad_imag = fourier(conj_real, conj_imag, cos_table, back_sin)
    layer_grads[0] = (probe[0] * grad_real + probe[1] * grad_imag, probe[0] * grad_imag - probe[1] * grad_real)
    probe_grad = jnp.stack([patch_real[:, 0] * grad_real + patch_imag[:, 0] * grad_imag, patch_real[:, 0] * grad_imag - patch_imag[:, 0] * grad_real], axis=1)
    lighting = patch_real[:, 0] * patch_real[:, 0] + patch_imag[:, 0] * patch_imag[:, 0]
    object_grad = jnp.stack([jnp.stack([item[0] for item in layer_grads], axis=1), jnp.stack([item[1] for item in layer_grads], axis=1)], axis=1)
    return (object_grad, probe_grad, lighting)

def reference(object_field, probe, kernel_phase, measured, positions, batch):
    side = probe.shape[-1]
    layers = object_field.shape[1]
    tables = dft_tables(side)
    kernel = (jnp.cos(kernel_phase), jnp.sin(kernel_phase))
    current = object_field
    beam = probe
    zero = jnp.zeros((), jnp.int32)
    for batch_no in range(BATCHES):

        def visit(carry, frame):
            grads, probe_sum, light_sum = carry
            where, amplitude, which = frame
            starts = (zero, zero, where[0].astype(jnp.int32), where[1].astype(jnp.int32))
            patch = lax.dynamic_slice(current, starts, (2, layers, side, side))
            object_grad, probe_grad, lighting = frame_pass(patch[None], beam, kernel, amplitude[None], tables)
            weight = (which == batch_no).astype(current.dtype)
            piece = lax.dynamic_slice(grads, starts, (2, layers, side, side)) + weight * object_grad[0]
            grads = lax.dynamic_update_slice(grads, piece, starts)
            return ((grads, probe_sum + weight * probe_grad[0], light_sum + weight * lighting[0]), None)
        start_carry = (jnp.zeros_like(current), jnp.zeros_like(beam), jnp.zeros((side, side), beam.dtype))
        (grads, probe_sum, light_sum), _ = lax.scan(visit, start_carry, (positions, measured, batch))
        peak = jnp.max(beam[0] * beam[0] + beam[1] * beam[1])
        current = current - grads / peak
        beam = beam - probe_sum / (light_sum + 1.0)
    return (current, beam)
```

```python
import math

import jax
import jax.numpy as jnp
import numpy as np
from jax import lax
from jax.experimental import pallas as pl
from jax.experimental.pallas import tpu as pltpu
from jax.sharding import PartitionSpec as P

BATCHES = 2
LANES = 128


def shifted(value, axis, steps):
    count = lax.axis_size(axis)
    first, last = (max(0, -steps), min(count, count - steps))
    return lax.ppermute(value, axis, [(source, source + steps) for source in range(first, last)])


def swapped(value, axis, step):
    count = lax.axis_size(axis)
    return lax.ppermute(value, axis, [(source, source ^ step) for source in range(count)])


def split_parts(table):
    high = table.astype(jnp.bfloat16)
    low = (table - high.astype(np.float32).astype(np.float64)).astype(jnp.bfloat16)
    return (high, low)


def dft_tables(side):
    half = side // 2
    index = np.arange(half)
    angle = 2.0 * math.pi * (index[:, None] * index[None, :] % half) / half
    cos, sin = (np.cos(angle) / math.sqrt(side), np.sin(angle) / math.sqrt(side))
    fore = np.block([[cos, -sin], [sin, cos]])
    back = np.block([[cos, sin], [-sin, cos]])
    fore_high, fore_low = split_parts(fore)
    back_high, back_low = split_parts(back)
    right = np.stack([np.concatenate([h, h, l], axis=0) for h, l in ((fore_high, fore_low), (back_high, back_low))])
    left = np.stack([np.concatenate([h, h, l], axis=1) for h, l in ((back_high, back_low), (fore_high, fore_low))])
    turn = 2.0 * math.pi * index / side
    twist = np.stack([np.cos(turn), -np.sin(turn)]).astype(np.float32)
    lane_twist = np.broadcast_to(twist[:, None, :], (2, 8, half))
    row_twist = np.broadcast_to(twist[:, :, None], (2, half, LANES))
    return tuple(jnp.asarray(np.ascontiguousarray(item)) for item in (right, left, lane_twist, row_twist))


def even_odd(value, axes):
    for axis in axes:
        shape = value.shape
        value = value.reshape(shape[:axis] + (shape[axis] // 2, 2) + shape[axis + 1 :])
        value = jnp.swapaxes(value, axis, axis + 1).reshape(shape)
    return value


def parts_of(value):
    high = value.astype(jnp.bfloat16)
    return (high, (value - high.astype(jnp.float32)).astype(jnp.bfloat16))


def dot(left, right):
    return jnp.dot(left, right, preferred_element_type=jnp.float32)


def by_rows(lead, table):
    high, low = parts_of(lead)
    return dot(jnp.concatenate([high, low, high], axis=1), table)


def by_columns(table, lead):
    high, low = parts_of(lead)
    return dot(table, jnp.concatenate([high, low, high], axis=0))


def lanes_forward(real, imag, table, twist):
    half = real.shape[1] // 2
    rows = real.shape[0]
    cos, sin = (twist[0, 0:1, :], twist[1, 0:1, :])
    sum_real, sum_imag = (real[:, :half] + real[:, half:], imag[:, :half] + imag[:, half:])
    gap_real, gap_imag = (real[:, :half] - real[:, half:], imag[:, :half] - imag[:, half:])
    odd_real, odd_imag = (gap_real * cos - gap_imag * sin, gap_real * sin + gap_imag * cos)
    lead = jnp.concatenate(
        [jnp.concatenate([sum_real, sum_imag], axis=1), jnp.concatenate([odd_real, odd_imag], axis=1)], axis=0
    )
    out = by_rows(lead, table)
    even, odd = (out[:rows], out[rows:])
    return (
        jnp.concatenate([even[:, :half], odd[:, :half]], axis=1),
        jnp.concatenate([even[:, half:], odd[:, half:]], axis=1),
    )


def lanes_inverse(real, imag, table, twist):
    half = real.shape[1] // 2
    rows = real.shape[0]
    cos, sin = (twist[0, 0:1, :], twist[1, 0:1, :])
    lead = jnp.concatenate(
        [
            jnp.concatenate([real[:, :half], imag[:, :half]], axis=1),
            jnp.concatenate([real[:, half:], imag[:, half:]], axis=1),
        ],
        axis=0,
    )
    out = by_rows(lead, table)
    even_real, even_imag = (out[:rows, :half], out[:rows, half:])
    odd_real, odd_imag = (out[rows:, :half], out[rows:, half:])
    turn_real, turn_imag = (odd_real * cos + odd_imag * sin, odd_imag * cos - odd_real * sin)
    return (
        jnp.concatenate([even_real + turn_real, even_real - turn_real], axis=1),
        jnp.concatenate([even_imag + turn_imag, even_imag - turn_imag], axis=1),
    )


def wide(twist, width):
    return jnp.concatenate([twist] * (width // twist.shape[1]), axis=1)


def rows_forward(real, imag, table, twist):
    half = real.shape[0] // 2
    cos, sin = (wide(twist[0], real.shape[1]), wide(twist[1], real.shape[1]))
    sum_real, sum_imag = (real[:half] + real[half:], imag[:half] + imag[half:])
    gap_real, gap_imag = (real[:half] - real[half:], imag[:half] - imag[half:])
    odd_real, odd_imag = (gap_real * cos - gap_imag * sin, gap_real * sin + gap_imag * cos)
    even = by_columns(table, jnp.concatenate([sum_real, sum_imag], axis=0))
    odd = by_columns(table, jnp.concatenate([odd_real, odd_imag], axis=0))
    return (
        jnp.concatenate([even[:half], odd[:half]], axis=0),
        jnp.concatenate([even[half:], odd[half:]], axis=0),
    )


def rows_inverse(real, imag, table, twist):
    half = real.shape[0] // 2
    cos, sin = (wide(twist[0], real.shape[1]), wide(twist[1], real.shape[1]))
    even = by_columns(table, jnp.concatenate([real[:half], imag[:half]], axis=0))
    odd = by_columns(table, jnp.concatenate([real[half:], imag[half:]], axis=0))
    odd_real, odd_imag = (odd[:half], odd[half:])
    turn_real, turn_imag = (odd_real * cos + odd_imag * sin, odd_imag * cos - odd_real * sin)
    return (
        jnp.concatenate([even[:half] + turn_real, even[:half] - turn_real], axis=0),
        jnp.concatenate([even[half:] + turn_imag, even[half:] - turn_imag], axis=0),
    )


CHUNK = 128


def chain(load, middle, store, side, work, right, left, lane_twist, row_twist):
    for start in range(0, side, CHUNK):
        rows = slice(start, start + CHUNK)
        real, imag = lanes_forward(*load(rows), right[0], lane_twist)
        work[0, rows, :] = real
        work[1, rows, :] = imag
    real, imag = rows_forward(work[0], work[1], left[0], row_twist)
    real, imag = middle(real, imag)
    real, imag = rows_inverse(real, imag, left[1], row_twist)
    work[0] = real
    work[1] = imag
    for start in range(0, side, CHUNK):
        rows = slice(start, start + CHUNK)
        store(rows, *lanes_inverse(work[0, rows, :], work[1, rows, :], right[1], lane_twist))


STRIP = 64
ROWS = 8


def numbers(groups, axis):
    return lax.broadcasted_iota(jnp.int32, (groups, ROWS, LANES), axis)


def bases(at, step):
    base = pl.multiple_of(at // step * step, step)
    return (base, at - base)


def cut(field, target, row, col, side):
    left, right = bases(col, LANES)
    top, under = bases(row, ROWS)
    groups = STRIP // ROWS
    take_rows = numbers(groups, 1) < ROWS - under
    take_cols = numbers(groups, 2) < LANES - right
    up, back = (lax.rem(ROWS - under, ROWS), lax.rem(LANES - right, LANES))

    def read(part, down, k):
        at = (part, pl.ds(pl.multiple_of(top + down, ROWS), STRIP + ROWS), pl.ds(pl.multiple_of(left + k * LANES, LANES), LANES))
        value = pltpu.roll(field[at], back, 1).reshape(groups + 1, ROWS, LANES)
        value = pltpu.roll(value, up, 1)
        return jnp.where(take_rows, value[:groups], value[1:])

    for part in range(field.shape[0]):

        @pl.loop(0, side // STRIP)
        def _(step):
            down = pl.multiple_of(step * STRIP, STRIP)
            turned = [read(part, down, k) for k in range(side // LANES + 1)]
            for k in range(side // LANES):
                value = jnp.where(take_cols, turned[k], turned[k + 1])
                target[part, pl.ds(down, STRIP), k * LANES : (k + 1) * LANES] = value.reshape(STRIP, LANES)


def place(field, source, row, col, side):
    left, right = bases(col, LANES)
    top, under = bases(row, ROWS)
    groups = STRIP // ROWS
    keep_rows = numbers(groups + 1, 1) >= under
    keep_cols = numbers(groups + 1, 2) >= right
    count = side // LANES
    edge = jnp.zeros((1, ROWS, LANES), jnp.float32)
    blank = jnp.zeros((groups + 1, ROWS, LANES), jnp.float32)

    def read(part, down, k):
        value = pltpu.roll(source[part, pl.ds(down, STRIP), k * LANES : (k + 1) * LANES], right, 1)
        value = pltpu.roll(value.reshape(groups, ROWS, LANES), under, 1)
        return jnp.where(
            keep_rows, jnp.concatenate([value, edge], axis=0), jnp.concatenate([edge, value], axis=0)
        )

    for part in range(field.shape[0]):

        @pl.loop(0, side // STRIP)
        def _(step):
            down = pl.multiple_of(step * STRIP, STRIP)
            turned = [blank] + [read(part, down, k) for k in range(count)] + [blank]
            for k in range(count + 1):
                value = jnp.where(keep_cols, turned[k + 1], turned[k]).reshape(STRIP + ROWS, LANES)
                spot = (
                    part,
                    pl.ds(pl.multiple_of(top + down, ROWS), STRIP + ROWS),
                    pl.ds(pl.multiple_of(left + k * LANES, LANES), LANES),
                )
                field[spot] = field[spot] + value


def block_spans(side, tile_rows, tile_cols):
    rows = [(0, side), (side, tile_rows - side), (tile_rows, side)]
    cols = [(0, side), (side, tile_cols - side), (tile_cols, side)]
    return [(r, c) for r in rows for c in cols]


def copies(blocks, field, spans, sem, outward):
    made = []
    for block, ((row, rows), (col, cols)) in zip(blocks, spans):
        window = field.at[:, pl.ds(row, rows), pl.ds(col, cols)]
        source, target = (window, block) if outward else (block, window)
        made.append(pltpu.make_async_copy(source, target, sem.at[len(made)]))
    return made


def run_all(items):
    for item in items:
        item.start()
    for item in items:
        item.wait()


def clear(field):
    rows = field.shape[1]

    @pl.loop(0, rows // 16)
    def _(step):
        at = pl.ds(pl.multiple_of(step * 16, 16), 16)
        for part in range(field.shape[0]):
            field[part, at, :] = jnp.zeros((16, field.shape[2]), jnp.float32)


def first_kernel(spans, side, slots, number, *refs):
    at, which, probe, phase, right, left, lane_twist, row_twist = refs[:8]
    blocks = refs[8:17]
    patches, incoming, field, work, sem = refs[17:]
    run_all(copies(blocks, field, spans, sem, False))

    @pl.loop(0, slots)
    def _(slot):
        @pl.when(which[slot] == number)
        def _():
            patch = patches.at[slot]
            out = incoming.at[slot]
            cut(field, patch, at[slot, 0], at[slot, 1], side)

            def load(rows):
                real, imag = (patch[0, rows, :], patch[1, rows, :])
                return (
                    probe[0, rows, :] * real - probe[1, rows, :] * imag,
                    probe[0, rows, :] * imag + probe[1, rows, :] * real,
                )

            def middle(real, imag):
                return (real * phase[0] - imag * phase[1], real * phase[1] + imag * phase[0])

            def store(rows, real, imag):
                out[0, rows, :] = real
                out[1, rows, :] = imag

            chain(load, middle, store, side, work, right, left, lane_twist, row_twist)


def second_kernel(spans, side, slots, number, *refs):
    at, which, incoming_all, measured, right, left, lane_twist, row_twist = refs[:8]
    blocks = refs[8:17]
    behind = refs[17]
    grads = refs[18:27]
    field, total, patch, delta, work, sem = refs[27:]
    moves = copies(blocks, field, spans, sem, False)
    for move in moves:
        move.start()
    clear(total)
    for move in moves:
        move.wait()

    @pl.loop(0, slots)
    def _(slot):
        @pl.when(which[slot] == number)
        def _():
            incoming = incoming_all.at[slot]
            out = behind.at[slot]
            cut(field, patch, at[slot, 0], at[slot, 1], side)

            def load(rows):
                real, imag = (patch[0, rows, :], patch[1, rows, :])
                in_real, in_imag = (incoming[0, rows, :], incoming[1, rows, :])
                return (real * in_real - imag * in_imag, real * in_imag + imag * in_real)

            def middle(real, imag):
                power = real * real + imag * imag
                factor = 1.0 - measured[slot] * lax.rsqrt(jnp.maximum(power, 0.01))
                return (real * factor, imag * factor)

            def store(rows, real, imag):
                in_real, in_imag = (incoming[0, rows, :], incoming[1, rows, :])
                delta[0, rows, :] = in_real * real + in_imag * imag
                delta[1, rows, :] = in_real * imag - in_imag * real
                own_real, own_imag = (patch[0, rows, :], patch[1, rows, :])
                out[0, rows, :] = own_real * real + own_imag * imag
                out[1, rows, :] = own_real * imag - own_imag * real

            chain(load, middle, store, side, work, right, left, lane_twist, row_twist)
            place(total, delta, at[slot, 0], at[slot, 1], side)

    run_all(copies(grads, total, spans, sem, True))


def third_kernel(spans, side, slots, number, *refs):
    at, which, probe, phase, patches, behind_all, right, left, lane_twist, row_twist = refs[:10]
    sums = refs[10]
    grads = refs[11:20]
    total, delta, work, sem = refs[20:]
    clear(total)
    sums[...] = jnp.zeros_like(sums)

    @pl.loop(0, slots)
    def _(slot):
        @pl.when(which[slot] == number)
        def _():
            behind = behind_all.at[slot]
            patch = patches.at[slot]

            def load(rows):
                return (behind[0, rows, :], behind[1, rows, :])

            def middle(real, imag):
                return (real * phase[0] + imag * phase[1], imag * phase[0] - real * phase[1])

            def store(rows, real, imag):
                in_real, in_imag = (probe[0, rows, :], probe[1, rows, :])
                delta[0, rows, :] = in_real * real + in_imag * imag
                delta[1, rows, :] = in_real * imag - in_imag * real
                own_real, own_imag = (patch[0, rows, :], patch[1, rows, :])
                sums[0, rows, :] = sums[0, rows, :] + (own_real * real + own_imag * imag)
                sums[1, rows, :] = sums[1, rows, :] + (own_real * imag - own_imag * real)
                sums[2, rows, :] = sums[2, rows, :] + (own_real * own_real + own_imag * own_imag)

            chain(load, middle, store, side, work, right, left, lane_twist, row_twist)
            place(total, delta, at[slot, 0], at[slot, 1], side)

    run_all(copies(grads, total, spans, sem, True))


VMEM = pltpu.MemorySpace.VMEM
SMEM = pltpu.MemorySpace.SMEM
ANY = pl.ANY


def spec(space):
    return pl.BlockSpec(memory_space=space)


def f32(*shape):
    return jax.ShapeDtypeStruct(shape, jnp.float32)


def quarters(field, side):
    return (
        field[:, :side, :side],
        field[:, :side, side:],
        field[:, side:, :side],
        field[:, side:, side:],
    )


def surroundings(own):
    low_left = shifted(own[0], "tile", -1)
    corner = shifted(low_left, "slab", -1)
    low_right = shifted(own[1], "tile", -1)
    top = shifted(own[0], "slab", -1)
    mid = shifted(own[2], "slab", -1)
    return (own[0], own[1], top, own[2], own[3], mid, low_left, low_right, corner)


def gathered(grads):
    low_right = shifted(grads[7], "tile", 1)
    corner = shifted(grads[8], "slab", 1)
    top = shifted(grads[2], "slab", 1)
    mid = shifted(grads[5], "slab", 1)
    low_left = shifted(grads[6] + corner, "tile", 1)
    return (grads[0] + top + low_left, grads[1] + low_right, grads[3] + mid, grads[4])


def new_probe(sums, beam):
    slab, tile = (lax.axis_size("slab"), lax.axis_size("tile"))
    order = [("slab", 1 << k) for k in range(slab.bit_length() - 1)]
    order += [("tile", 1 << k) for k in range(tile.bit_length() - 1)]
    cuts = [item for item in order if item[0] == "slab" or item[1] == 1]
    rest = [item for item in order if item not in cuts]
    value = sums
    mine = beam
    for axis, step in cuts:
        upper = (lax.axis_index(axis) & step) != 0
        half = value.shape[1] // 2
        first, last = (value[:, :half], value[:, half:])
        got = swapped(jnp.where(upper, first, last), axis, step)
        value = jnp.where(upper, last, first) + got
        mine = jnp.where(upper, mine[:, half:], mine[:, :half])
    for axis, step in rest:
        value = value + swapped(value, axis, step)
    mine = mine - value[:2] / (value[2] + 1.0)
    for axis, step in cuts[::-1]:
        upper = (lax.axis_index(axis) & step) != 0
        got = swapped(mine, axis, step)
        mine = jnp.concatenate([jnp.where(upper, got, mine), jnp.where(upper, mine, got)], axis=1)
    return mine


def shards(object_field, probe, kernel_phase, measured, positions, batch):
    side = probe.shape[-1]
    tile_rows, tile_cols = object_field.shape[2:]
    slots = positions.shape[0]
    tables = dft_tables(side)
    spans = block_spans(side, tile_rows, tile_cols)
    turned = even_odd(kernel_phase, (0, 1))
    phase = jnp.stack([jnp.cos(turned), jnp.sin(turned)])
    amplitude = even_odd(measured, (1, 2))
    corner = jnp.stack([lax.axis_index("tile") * tile_rows, lax.axis_index("slab") * tile_cols])
    local_at = positions - corner[None, :]
    frames = f32(slots, 2, side, side)
    block_shapes = [f32(2, rows, cols) for (_, rows), (_, cols) in spans]
    whole = pltpu.VMEM((2, tile_rows + side, tile_cols + side), jnp.float32)
    plane = pltpu.VMEM((2, side, side), jnp.float32)
    sems = pltpu.SemaphoreType.DMA((len(spans),))
    smem2 = [spec(SMEM)] * 2
    nine = [spec(ANY)] * len(spans)
    cost = pl.CostEstimate(flops=int(slots * 40e9), bytes_accessed=16 << 20, transcendentals=0)
    params = pltpu.CompilerParams(vmem_limit_bytes=48 << 20)

    def call(body, number, ins, outs, out_shapes, scratch, name):
        def run(*refs):
            body(spans, side, slots, number, *refs)

        return pl.pallas_call(
            run,
            in_specs=ins,
            out_specs=outs,
            out_shape=out_shapes,
            scratch_shapes=scratch,
            cost_estimate=cost,
            compiler_params=params,
            name=name,
        )

    layers = [quarters(object_field[:, layer], side) for layer in range(2)]
    beam = probe
    for number in range(BATCHES):
        around = [surroundings(layer) for layer in layers]
        patches, incoming = call(
            first_kernel,
            number,
            smem2 + [spec(VMEM)] * 6 + nine,
            [spec(VMEM)] * 2,
            [frames, frames],
            [whole, plane, sems],
            f"first{number}",
        )(local_at, batch, beam, phase, *tables, *around[0])
        behind, *grads1 = call(
            second_kernel,
            number,
            smem2 + [spec(VMEM)] * 6 + nine,
            [spec(VMEM)] + nine,
            [frames] + block_shapes,
            [whole, whole, plane, plane, plane, sems],
            f"second{number}",
        )(local_at, batch, incoming, amplitude, *tables, *around[1])
        sums, *grads0 = call(
            third_kernel,
            number,
            smem2 + [spec(VMEM)] * 8,
            [spec(VMEM)] + nine,
            [f32(3, side, side)] + block_shapes,
            [whole, plane, plane, sems],
            f"third{number}",
        )(local_at, batch, beam, phase, patches, behind, *tables)
        peak = jnp.max(beam[0] * beam[0] + beam[1] * beam[1])
        sum1 = gathered(grads1)
        sum0 = gathered(grads0)
        layers = [
            tuple(old - new / peak for old, new in zip(layer, total)) for layer, total in zip(layers, (sum0, sum1))
        ]
        beam = new_probe(sums, beam)
    stacked = jnp.stack(
        [
            jnp.concatenate(
                [jnp.concatenate([a, b], axis=2), jnp.concatenate([c, d], axis=2)],
                axis=1,
            )
            for a, b, c, d in layers
        ],
        axis=1,
    )
    return (stacked, beam)


def solution(mesh):
    in_specs = (
        P(None, None, "tile", "slab"),
        P(),
        P(),
        P(("tile", "slab"), None, None),
        P(("tile", "slab"), None),
        P(("tile", "slab")),
    )
    out_specs = (P(None, None, "tile", "slab"), P())
    return jax.shard_map(shards, mesh=mesh, in_specs=in_specs, out_specs=out_specs, check_vma=False)
```

```python
import math

import jax
import jax.numpy as jnp
import numpy as np
from jax import lax
from jax.experimental import pallas as pl
from jax.experimental.pallas import tpu as pltpu
from jax.sharding import PartitionSpec as P


BATCHES = 2
LANES = 128


def shifted(value, axis, steps):
    count = lax.axis_size(axis)
    first, last = (max(0, -steps), min(count, count - steps))
    return lax.ppermute(value, axis, [(source, source + steps) for source in range(first, last)])


def swapped(value, axis, step):
    count = lax.axis_size(axis)
    return lax.ppermute(value, axis, [(source, source ^ step) for source in range(count)])


def split_parts(table):
    high = table.astype(jnp.bfloat16)
    low = (table - high.astype(np.float32).astype(np.float64)).astype(jnp.bfloat16)
    return (high, low)


def dft_tables(side):
    half = side // 2
    index = np.arange(half)
    angle = 2.0 * math.pi * (index[:, None] * index[None, :] % half) / half
    cos, sin = (np.cos(angle) / math.sqrt(side), np.sin(angle) / math.sqrt(side))
    fore = np.block([[cos, -sin], [sin, cos]])
    back = np.block([[cos, sin], [-sin, cos]])
    fore_high, fore_low = split_parts(fore)
    back_high, back_low = split_parts(back)
    right = np.stack([np.concatenate([h, l], axis=0) for h, l in ((fore_high, fore_low), (back_high, back_low))])
    left = np.stack([np.concatenate([h, l], axis=1) for h, l in ((back_high, back_low), (fore_high, fore_low))])
    turn = 2.0 * math.pi * index / side
    twist = np.stack([np.cos(turn), -np.sin(turn)]).astype(np.float32)
    lane_twist = np.broadcast_to(twist[:, None, :], (2, 8, half))
    row_twist = np.broadcast_to(twist[:, :, None], (2, half, LANES))
    return tuple(jnp.asarray(np.ascontiguousarray(item)) for item in (right, left, lane_twist, row_twist))


def parts_of(value):
    high = value.astype(jnp.bfloat16)
    return (high, (value - high.astype(jnp.float32)).astype(jnp.bfloat16))


def dot(left, right):
    return jnp.dot(left, right, preferred_element_type=jnp.float32)


def by_rows(lead, table):
    high, low = parts_of(lead)
    side = table.shape[0] // 2
    table = jnp.concatenate([table[:side], table], axis=0)
    return dot(jnp.concatenate([high, low, high], axis=1), table)


def by_columns(table, lead):
    high, low = parts_of(lead)
    side = table.shape[1] // 2
    table = jnp.concatenate([table[:, :side], table], axis=1)
    return dot(table, jnp.concatenate([high, low, high], axis=0))


def lanes_forward(real, imag, table, twist):
    half = real.shape[1] // 2
    rows = real.shape[0]
    cos, sin = (twist[0, 0:1, :], twist[1, 0:1, :])
    sum_real, sum_imag = (real[:, :half] + real[:, half:], imag[:, :half] + imag[:, half:])
    gap_real, gap_imag = (real[:, :half] - real[:, half:], imag[:, :half] - imag[:, half:])
    odd_real, odd_imag = (gap_real * cos - gap_imag * sin, gap_real * sin + gap_imag * cos)
    lead = jnp.concatenate(
        [jnp.concatenate([sum_real, sum_imag], axis=1), jnp.concatenate([odd_real, odd_imag], axis=1)], axis=0
    )
    out = by_rows(lead, table)
    even, odd = (out[:rows], out[rows:])
    return (
        jnp.concatenate([even[:, :half], odd[:, :half]], axis=1),
        jnp.concatenate([even[:, half:], odd[:, half:]], axis=1),
    )


def lanes_inverse(real, imag, table, twist):
    half = real.shape[1] // 2
    rows = real.shape[0]
    cos, sin = (twist[0, 0:1, :], twist[1, 0:1, :])
    lead = jnp.concatenate(
        [
            jnp.concatenate([real[:, :half], imag[:, :half]], axis=1),
            jnp.concatenate([real[:, half:], imag[:, half:]], axis=1),
        ],
        axis=0,
    )
    out = by_rows(lead, table)
    even_real, even_imag = (out[:rows, :half], out[:rows, half:])
    odd_real, odd_imag = (out[rows:, :half], out[rows:, half:])
    turn_real, turn_imag = (odd_real * cos + odd_imag * sin, odd_imag * cos - odd_real * sin)
    return (
        jnp.concatenate([even_real + turn_real, even_real - turn_real], axis=1),
        jnp.concatenate([even_imag + turn_imag, even_imag - turn_imag], axis=1),
    )


def wide(twist, width):
    return jnp.concatenate([twist] * (width // twist.shape[1]), axis=1)


def rows_forward(real, imag, table, twist):
    half = real.shape[0] // 2
    cos, sin = (wide(twist[0], real.shape[1]), wide(twist[1], real.shape[1]))
    sum_real, sum_imag = (real[:half] + real[half:], imag[:half] + imag[half:])
    gap_real, gap_imag = (real[:half] - real[half:], imag[:half] - imag[half:])
    odd_real, odd_imag = (gap_real * cos - gap_imag * sin, gap_real * sin + gap_imag * cos)
    even = by_columns(table, jnp.concatenate([sum_real, sum_imag], axis=0))
    odd = by_columns(table, jnp.concatenate([odd_real, odd_imag], axis=0))
    return (
        jnp.concatenate([even[:half], odd[:half]], axis=0),
        jnp.concatenate([even[half:], odd[half:]], axis=0),
    )


def rows_inverse(real, imag, table, twist):
    half = real.shape[0] // 2
    cos, sin = (wide(twist[0], real.shape[1]), wide(twist[1], real.shape[1]))
    even = by_columns(table, jnp.concatenate([real[:half], imag[:half]], axis=0))
    odd = by_columns(table, jnp.concatenate([real[half:], imag[half:]], axis=0))
    odd_real, odd_imag = (odd[:half], odd[half:])
    turn_real, turn_imag = (odd_real * cos + odd_imag * sin, odd_imag * cos - odd_real * sin)
    return (
        jnp.concatenate([even[:half] + turn_real, even[:half] - turn_real], axis=0),
        jnp.concatenate([even[half:] + turn_imag, even[half:] - turn_imag], axis=0),
    )


CHUNK = 128


def chain(load, middle, store, side, work, right, left, lane_twist, row_twist):
    for start in range(0, side, CHUNK):
        rows = slice(start, start + CHUNK)
        real, imag = lanes_forward(*load(rows), right[0], lane_twist)
        work[0, rows, :] = real
        work[1, rows, :] = imag
    real, imag = rows_forward(work[0], work[1], left[0], row_twist)
    real, imag = middle(real, imag)
    real, imag = rows_inverse(real, imag, left[1], row_twist)
    work[0] = real
    work[1] = imag

    for start in range(0, side, CHUNK):
        rows = slice(start, start + CHUNK)
        store(rows, *lanes_inverse(work[0, rows, :], work[1, rows, :], right[1], lane_twist))


STRIP = 64
ROWS = 8


def numbers(groups, axis):
    return lax.broadcasted_iota(jnp.int32, (groups, ROWS, LANES), axis)


def bases(at, step):
    base = pl.multiple_of(at // step * step, step)
    return (base, at - base)


def cut(field, target, row, col, side):
    left, right = bases(col, LANES)
    top, under = bases(row, ROWS)
    groups = STRIP // ROWS
    take_rows = numbers(groups, 1) < ROWS - under
    take_cols = numbers(groups, 2) < LANES - right
    up, back = (lax.rem(ROWS - under, ROWS), lax.rem(LANES - right, LANES))

    def read(part, down, k):
        at = (part, pl.ds(pl.multiple_of(top + down, ROWS), STRIP + ROWS), pl.ds(pl.multiple_of(left + k * LANES, LANES), LANES))
        value = pltpu.roll(field[at], back, 1).reshape(groups + 1, ROWS, LANES)
        value = pltpu.roll(value, up, 1)
        return jnp.where(take_rows, value[:groups], value[1:])

    for part in range(field.shape[0]):

        @pl.loop(0, side // STRIP)
        def _(step):
            down = pl.multiple_of(step * STRIP, STRIP)
            turned = [read(part, down, k) for k in range(side // LANES + 1)]
            for k in range(side // LANES):
                value = jnp.where(take_cols, turned[k], turned[k + 1])
                target[part, pl.ds(down, STRIP), k * LANES : (k + 1) * LANES] = value.reshape(STRIP, LANES)


def place(field, source, row, col, side):
    left, right = bases(col, LANES)
    top, under = bases(row, ROWS)
    groups = STRIP // ROWS
    keep_rows = numbers(groups + 1, 1) >= under
    keep_cols = numbers(groups + 1, 2) >= right
    count = side // LANES
    edge = jnp.zeros((1, ROWS, LANES), jnp.float32)
    blank = jnp.zeros((groups + 1, ROWS, LANES), jnp.float32)

    def read(part, down, k):
        value = pltpu.roll(source[part, pl.ds(down, STRIP), k * LANES : (k + 1) * LANES], right, 1)
        value = pltpu.roll(value.reshape(groups, ROWS, LANES), under, 1)
        return jnp.where(
            keep_rows, jnp.concatenate([value, edge], axis=0), jnp.concatenate([edge, value], axis=0)
        )

    for part in range(field.shape[0]):

        @pl.loop(0, side // STRIP)
        def _(step):
            down = pl.multiple_of(step * STRIP, STRIP)
            turned = [blank] + [read(part, down, k) for k in range(count)] + [blank]
            for k in range(count + 1):
                value = jnp.where(keep_cols, turned[k + 1], turned[k]).reshape(STRIP + ROWS, LANES)
                spot = (
                    part,
                    pl.ds(pl.multiple_of(top + down, ROWS), STRIP + ROWS),
                    pl.ds(pl.multiple_of(left + k * LANES, LANES), LANES),
                )
                field[spot] = field[spot] + value


def halo_spans(side, rows, cols):
    return [
        (0, cols, side, side),
        (side, cols, rows - side, side),
        (rows, 0, side, side),
        (rows, side, side, cols - side),
        (rows, cols, side, side),
    ]


def own_spans(side, rows, cols):
    rest_rows, rest_cols = (rows - side, cols - side)
    return [
        (0, 0, side, side),
        (0, side, side, rest_cols),
        (side, 0, rest_rows, side),
        (side, side, rest_rows, rest_cols),
    ]


def grad_spans(side, rows, cols):
    return own_spans(side, rows, cols) + [
        (0, cols, rows, side),
        (rows, side, side, cols - side),
        (rows, 0, side, side),
        (rows, cols, side, side),
    ]


def copies(blocks, field, spans, sem, outward):
    made = []
    for block, (row, col, rows, cols) in zip(blocks, spans):
        window = field.at[:, pl.ds(row, rows), pl.ds(col, cols)]
        source, target = (window, block) if outward else (block, window)
        made.append(pltpu.make_async_copy(source, target, sem.at[len(made)]))
    return made


def start_all(items):
    for item in items:
        item.start()


def wait_all(items):
    for item in items:
        item.wait()


def clear(field):
    rows = field.shape[1]

    @pl.loop(0, rows // 16)
    def _(step):
        at = pl.ds(pl.multiple_of(step * 16, 16), 16)
        for part in range(field.shape[0]):
            field[part, at, :] = jnp.zeros((16, field.shape[2]), jnp.float32)


def three_parts(value, axis):
    high = value.astype(jnp.bfloat16)
    rest = value - high.astype(jnp.float32)
    mid = rest.astype(jnp.bfloat16)
    low = (rest - mid.astype(jnp.float32)).astype(jnp.bfloat16)
    return jnp.concatenate([high, mid, low], axis=axis)


def even_odd(value):
    side = value.shape[0]
    first, second = (lax.broadcasted_iota(jnp.int32, (side, side), axis) for axis in (0, 1))

    def table(source, target):
        at = jnp.where(target < side // 2, 2 * target, 2 * target - side + 1)
        return jnp.where(source == at, 1.0, 0.0).astype(jnp.bfloat16)

    right, left = (table(first, second), table(second, first))
    value = dot(three_parts(value, 1), jnp.concatenate([right] * 3, axis=0))
    return dot(jnp.concatenate([left] * 3, axis=1), three_parts(value, 0))


def sort_kernel(side, slots, number, measured, angle, amplitude, phase):
    turned = even_odd(angle[...])
    phase[0] = jnp.cos(turned)
    phase[1] = jnp.sin(turned)

    @pl.loop(0, slots)
    def _(slot):
        amplitude[slot] = even_odd(measured[slot])


def sources(refs, spans, layer):
    if len(refs) < len(spans):
        tile = refs[0].at[:, layer]
        return ([tile, *refs[1:]], [(0, 0, *tile.shape[1:]), *spans[4:]])
    return (refs, spans)


def first_kernel(spans, side, slots, number, *refs):
    at, which, probe, phase, right, left, lane_twist, row_twist = refs[:8]
    patches, incoming, field, work, sem = refs[-5:]
    blocks, places = sources(refs[8:-5], spans, 0)
    moves = copies(blocks, field, places, sem, False)
    start_all(moves)
    wait_all(moves)

    @pl.loop(0, slots)
    def _(slot):
        @pl.when(which[slot] == number)
        def _():
            patch = patches.at[slot]
            out = incoming.at[slot]
            cut(field, patch, at[slot, 0], at[slot, 1], side)

            def load(rows):
                real, imag = (patch[0, rows, :], patch[1, rows, :])
                return (
                    probe[0, rows, :] * real - probe[1, rows, :] * imag,
                    probe[0, rows, :] * imag + probe[1, rows, :] * real,
                )

            def middle(real, imag):
                return (real * phase[0] - imag * phase[1], real * phase[1] + imag * phase[0])

            def store(rows, real, imag):
                out[0, rows, :] = real
                out[1, rows, :] = imag

            chain(load, middle, store, side, work, right, left, lane_twist, row_twist)


def second_kernel(spans, side, slots, number, *refs):
    at, which, probe, phase, patches, incoming_all, measured, right, left, lane_twist, row_twist = refs[:11]
    sums, *grads = refs[-18:-9]
    field, total1, total0, patch, delta, behind_all, work, sem, sem_out = refs[-9:]
    rows, cols = (total0.shape[1] - side, total0.shape[2] - side)
    places_out = grad_spans(side, rows, cols)
    blocks, places = sources(refs[11:-18], spans, 1)
    moves = copies(blocks, field, places, sem, False)
    start_all(moves)
    clear(total1)
    clear(total0)
    sums[...] = jnp.zeros_like(sums)
    wait_all(moves)

    @pl.loop(0, slots)
    def _(slot):
        @pl.when(which[slot] == number)
        def _():
            incoming = incoming_all.at[slot]
            out = behind_all.at[slot]
            cut(field, patch, at[slot, 0], at[slot, 1], side)

            def load(rows):
                real, imag = (patch[0, rows, :], patch[1, rows, :])
                in_real, in_imag = (incoming[0, rows, :], incoming[1, rows, :])
                return (real * in_real - imag * in_imag, real * in_imag + imag * in_real)

            def middle(real, imag):
                power = real * real + imag * imag
                factor = 1.0 - measured[slot] * lax.rsqrt(jnp.maximum(power, 0.01))
                return (real * factor, imag * factor)

            def store(rows, real, imag):
                in_real, in_imag = (incoming[0, rows, :], incoming[1, rows, :])
                delta[0, rows, :] = in_real * real + in_imag * imag
                delta[1, rows, :] = in_real * imag - in_imag * real
                own_real, own_imag = (patch[0, rows, :], patch[1, rows, :])
                out[0, rows, :] = own_real * real + own_imag * imag
                out[1, rows, :] = own_real * imag - own_imag * real

            chain(load, middle, store, side, work, right, left, lane_twist, row_twist)
            place(total1, delta, at[slot, 0], at[slot, 1], side)

    moves1 = copies([grad.at[1] for grad in grads], total1, places_out, sem, True)
    start_all(moves1)

    @pl.loop(0, slots)
    def _(slot):
        @pl.when(which[slot] == number)
        def _():
            behind = behind_all.at[slot]
            first = patches.at[slot]

            def load(rows):
                return (behind[0, rows, :], behind[1, rows, :])

            def middle(real, imag):
                return (real * phase[0] + imag * phase[1], imag * phase[0] - real * phase[1])

            def store(rows, real, imag):
                in_real, in_imag = (probe[0, rows, :], probe[1, rows, :])
                delta[0, rows, :] = in_real * real + in_imag * imag
                delta[1, rows, :] = in_real * imag - in_imag * real
                own_real, own_imag = (first[0, rows, :], first[1, rows, :])
                sums[0, rows, :] = sums[0, rows, :] + (own_real * real + own_imag * imag)
                sums[1, rows, :] = sums[1, rows, :] + (own_real * imag - own_imag * real)
                sums[2, rows, :] = sums[2, rows, :] + (own_real * own_real + own_imag * own_imag)

            chain(load, middle, store, side, work, right, left, lane_twist, row_twist)
            place(total0, delta, at[slot, 0], at[slot, 1], side)

    moves0 = copies([grad.at[0] for grad in grads], total0, places_out, sem_out, True)
    start_all(moves0)
    wait_all(moves1)
    wait_all(moves0)


VMEM = pltpu.MemorySpace.VMEM
SMEM = pltpu.MemorySpace.SMEM
ANY = pl.ANY


def spec(space):
    return pl.BlockSpec(memory_space=space)


def f32(*shape):
    return jax.ShapeDtypeStruct(shape, jnp.float32)


def quarters(field, side):
    return (
        field[:, :side, :side],
        field[:, :side, side:],
        field[:, side:, :side],
        field[:, side:, side:],
    )


def surroundings(own):
    low_left = shifted(own[0], "tile", -1)
    corner = shifted(low_left, "slab", -1)
    low_right = shifted(own[1], "tile", -1)
    top = shifted(own[0], "slab", -1)
    mid = shifted(own[2], "slab", -1)
    return [top, mid, low_left, low_right, corner]


def gathered(grads):
    low_right = shifted(grads[5], "tile", 1)
    corner = shifted(grads[7], "slab", 1)
    right = shifted(grads[4], "slab", 1)
    side = corner.shape[2]
    layers = []
    for layer in range(corner.shape[0]):
        low_left = shifted(grads[6][layer] + corner[layer], "tile", 1)
        layers.append(
            (
                grads[0][layer] + right[layer, :, :side] + low_left,
                grads[1][layer] + low_right[layer],
                grads[2][layer] + right[layer, :, side:],
                grads[3][layer],
            )
        )
    return layers


def stepped(layer, total, peak):
    new = [None] * len(layer)
    for block in (3, 1, 2, 0):
        new[block] = layer[block] - total[block] / peak
        peak, new[block] = lax.optimization_barrier((peak, new[block]))
    return tuple(new)


def doublings(axis):
    return [(axis, 1 << k) for k in range(lax.axis_size(axis).bit_length() - 1)]


def new_probe(sums, beam):
    tile = doublings("tile")
    cuts, rest = (doublings("slab") + tile[1:], tile[:1])
    value = sums
    mine = beam
    for axis, step in cuts:
        upper = (lax.axis_index(axis) & step) != 0
        half = value.shape[1] // 2
        first, last = (value[:, :half], value[:, half:])
        got = swapped(jnp.where(upper, first, last), axis, step)
        value = jnp.where(upper, last, first) + got
        mine = jnp.where(upper, mine[:, half:], mine[:, :half])
    for axis, step in rest:
        value = value + swapped(value, axis, step)
    mine = mine - value[:2] / (value[2] + 1.0)
    for axis, step in cuts[::-1]:
        upper = (lax.axis_index(axis) & step) != 0
        got = swapped(mine, axis, step)
        mine = jnp.concatenate([jnp.where(upper, got, mine), jnp.where(upper, mine, got)], axis=1)
    return mine


def update(object_field, probe, kernel_phase, measured, positions, batch):
    side = probe.shape[-1]
    tile_rows, tile_cols = object_field.shape[2:]
    slots = positions.shape[0]
    tables = dft_tables(side)
    spans = own_spans(side, tile_rows, tile_cols) + halo_spans(side, tile_rows, tile_cols)
    places_out = grad_spans(side, tile_rows, tile_cols)
    corner = jnp.stack([lax.axis_index("tile") * tile_rows, lax.axis_index("slab") * tile_cols])
    local_at = positions - corner[None, :]
    frames = f32(slots, 2, side, side)
    grad_shapes = [f32(2, 2, rows, cols) for _, _, rows, cols in places_out]
    whole = pltpu.VMEM((2, tile_rows + side, tile_cols + side), jnp.float32)
    plane = pltpu.VMEM((2, side, side), jnp.float32)
    sems = pltpu.SemaphoreType.DMA((len(spans),))
    smem2 = [spec(SMEM)] * 2
    out_sems = pltpu.SemaphoreType.DMA((len(places_out),))
    cost = pl.CostEstimate(flops=int(slots * 40e9), bytes_accessed=16 << 20, transcendentals=0)
    params = pltpu.CompilerParams(vmem_limit_bytes=48 << 20)

    def call(body, given, number, ins, outs, out_shapes, scratch):
        def run(*refs):
            body(*given, side, slots, number, *refs)

        return pl.pallas_call(
            run,
            in_specs=ins,
            out_specs=outs,
            out_shape=out_shapes,
            scratch_shapes=scratch,
            cost_estimate=cost,
            compiler_params=params,
        )

    amplitude, phase = call(
        sort_kernel, (), 0, [spec(VMEM)] * 2, [spec(VMEM)] * 2, [f32(slots, side, side), f32(2, side, side)], []
    )(measured, kernel_phase)
    layers = [quarters(object_field[:, layer], side) for layer in range(2)]
    beam = probe
    for number in range(BATCHES):
        around = [surroundings(layers[k]) for k in range(2)]
        owns = [[object_field] if number == 0 else list(layer) for layer in layers]
        fields = [own + halo for own, halo in zip(owns, around)]
        counts = [len(field) for field in fields]
        patches, incoming = call(
            first_kernel,
            (spans,),
            number,
            smem2 + [spec(VMEM)] * 6 + [spec(ANY)] * counts[0],
            [spec(VMEM)] * 2,
            [frames, frames],
            [whole, plane, sems],
        )(local_at, batch, beam, phase, *tables, *fields[0])
        sums, *grads = call(
            second_kernel,
            (spans,),
            number,
            smem2 + [spec(VMEM)] * 9 + [spec(ANY)] * counts[1],
            [spec(VMEM)] + [spec(ANY)] * len(grad_shapes),
            [f32(3, side, side)] + grad_shapes,
            [whole, whole, whole, plane, plane, pltpu.VMEM(frames.shape, jnp.float32), plane, sems, out_sems],
        )(local_at, batch, beam, phase, patches, incoming, amplitude, *tables, *fields[1])
        peak = jnp.max(beam[0] * beam[0] + beam[1] * beam[1])
        total = gathered(grads)
        layers = [stepped(layers[k], total[k], peak) for k in range(2)]
        beam = new_probe(sums, beam)
    result = jnp.zeros((2, 2 * tile_rows, tile_cols), jnp.float32)
    for block in (3, 1, 2, 0):
        for layer in (0, 1):
            row, col, _, _ = spans[block]
            result = lax.dynamic_update_slice(result, layers[layer][block], (0, layer * tile_rows + row, col))
    result = result.reshape(object_field.shape)
    return (result, beam)


def solution(mesh):
    in_specs = (
        P(None, None, "tile", "slab"),
        P(),
        P(),
        P(("tile", "slab"), None, None),
        P(("tile", "slab"), None),
        P(("tile", "slab")),
    )
    out_specs = (P(None, None, "tile", "slab"), P())
    return jax.shard_map(update, mesh=mesh, in_specs=in_specs, out_specs=out_specs, check_vma=False)
```

```python
import math

import jax
import jax.numpy as jnp
import numpy as np
from jax import lax
from jax.experimental import pallas as pl
from jax.experimental.pallas import tpu as pltpu
from jax.sharding import PartitionSpec as P


BATCHES = 2
LANES = 128


def shifted(value, axis, steps):
    count = lax.axis_size(axis)
    first, last = (max(0, -steps), min(count, count - steps))
    return lax.ppermute(value, axis, [(source, source + steps) for source in range(first, last)])


def swapped(value, axis, step):
    count = lax.axis_size(axis)
    return lax.ppermute(value, axis, [(source, source ^ step) for source in range(count)])


def split_parts(table):
    high = table.astype(jnp.bfloat16)
    low = (table - high.astype(np.float32).astype(np.float64)).astype(jnp.bfloat16)
    return (high, low)


def dft_tables(side):
    half = side // 2
    index = np.arange(half)
    angle = 2.0 * math.pi * (index[:, None] * index[None, :] % half) / half
    cos, sin = (np.cos(angle) / math.sqrt(side), np.sin(angle) / math.sqrt(side))
    fore = np.block([[cos, -sin], [sin, cos]])
    back = np.block([[cos, sin], [-sin, cos]])
    fore_high, fore_low = split_parts(fore)
    back_high, back_low = split_parts(back)
    right = np.stack([np.concatenate([h, l], axis=0) for h, l in ((fore_high, fore_low), (back_high, back_low))])
    left = np.stack([np.concatenate([h, l], axis=1) for h, l in ((back_high, back_low), (fore_high, fore_low))])
    turn = 2.0 * math.pi * index / side
    twist = np.stack([np.cos(turn), -np.sin(turn)]).astype(np.float32)
    lane_twist = np.broadcast_to(twist[:, None, :], (2, 8, half))
    row_twist = np.broadcast_to(twist[:, :, None], (2, half, LANES))
    return tuple(jnp.asarray(np.ascontiguousarray(item)) for item in (right, left, lane_twist, row_twist))


def parts_of(value):
    high = value.astype(jnp.bfloat16)
    return (high, (value - high.astype(jnp.float32)).astype(jnp.bfloat16))


def dot(left, right):
    return jnp.dot(left, right, preferred_element_type=jnp.float32)


def by_rows(lead, table):
    high, low = parts_of(lead)
    side = table.shape[0] // 2
    table = jnp.concatenate([table[:side], table], axis=0)
    return dot(jnp.concatenate([high, low, high], axis=1), table)


def by_columns(table, lead):
    high, low = parts_of(lead)
    side = table.shape[1] // 2
    table = jnp.concatenate([table[:, :side], table], axis=1)
    return dot(table, jnp.concatenate([high, low, high], axis=0))


def lanes_forward(real, imag, table, twist):
    half = real.shape[1] // 2
    rows = real.shape[0]
    cos, sin = (twist[0, 0:1, :], twist[1, 0:1, :])
    sum_real, sum_imag = (real[:, :half] + real[:, half:], imag[:, :half] + imag[:, half:])
    gap_real, gap_imag = (real[:, :half] - real[:, half:], imag[:, :half] - imag[:, half:])
    odd_real, odd_imag = (gap_real * cos - gap_imag * sin, gap_real * sin + gap_imag * cos)
    lead = jnp.concatenate(
        [jnp.concatenate([sum_real, sum_imag], axis=1), jnp.concatenate([odd_real, odd_imag], axis=1)], axis=0
    )
    out = by_rows(lead, table)
    even, odd = (out[:rows], out[rows:])
    return (
        jnp.concatenate([even[:, :half], odd[:, :half]], axis=1),
        jnp.concatenate([even[:, half:], odd[:, half:]], axis=1),
    )


def lanes_inverse(real, imag, table, twist):
    half = real.shape[1] // 2
    rows = real.shape[0]
    cos, sin = (twist[0, 0:1, :], twist[1, 0:1, :])
    lead = jnp.concatenate(
        [
            jnp.concatenate([real[:, :half], imag[:, :half]], axis=1),
            jnp.concatenate([real[:, half:], imag[:, half:]], axis=1),
        ],
        axis=0,
    )
    out = by_rows(lead, table)
    even_real, even_imag = (out[:rows, :half], out[:rows, half:])
    odd_real, odd_imag = (out[rows:, :half], out[rows:, half:])
    turn_real, turn_imag = (odd_real * cos + odd_imag * sin, odd_imag * cos - odd_real * sin)
    return (
        jnp.concatenate([even_real + turn_real, even_real - turn_real], axis=1),
        jnp.concatenate([even_imag + turn_imag, even_imag - turn_imag], axis=1),
    )


def wide(twist, width):
    return jnp.concatenate([twist] * (width // twist.shape[1]), axis=1)


def rows_forward(real, imag, table, twist):
    half = real.shape[0] // 2
    cos, sin = (wide(twist[0], real.shape[1]), wide(twist[1], real.shape[1]))
    sum_real, sum_imag = (real[:half] + real[half:], imag[:half] + imag[half:])
    gap_real, gap_imag = (real[:half] - real[half:], imag[:half] - imag[half:])
    odd_real, odd_imag = (gap_real * cos - gap_imag * sin, gap_real * sin + gap_imag * cos)
    even = by_columns(table, jnp.concatenate([sum_real, sum_imag], axis=0))
    odd = by_columns(table, jnp.concatenate([odd_real, odd_imag], axis=0))
    return (
        jnp.concatenate([even[:half], odd[:half]], axis=0),
        jnp.concatenate([even[half:], odd[half:]], axis=0),
    )


def rows_inverse(real, imag, table, twist):
    half = real.shape[0] // 2
    cos, sin = (wide(twist[0], real.shape[1]), wide(twist[1], real.shape[1]))
    even = by_columns(table, jnp.concatenate([real[:half], imag[:half]], axis=0))
    odd = by_columns(table, jnp.concatenate([real[half:], imag[half:]], axis=0))
    odd_real, odd_imag = (odd[:half], odd[half:])
    turn_real, turn_imag = (odd_real * cos + odd_imag * sin, odd_imag * cos - odd_real * sin)
    return (
        jnp.concatenate([even[:half] + turn_real, even[:half] - turn_real], axis=0),
        jnp.concatenate([even[half:] + turn_imag, even[half:] - turn_imag], axis=0),
    )


CHUNK = 128


def chain(load, middle, store, side, work, right, left, lane_twist, row_twist):
    for start in range(0, side, CHUNK):
        rows = slice(start, start + CHUNK)
        real, imag = lanes_forward(*load(rows), right[0], lane_twist)
        work[0, rows, :] = real
        work[1, rows, :] = imag
    real, imag = rows_forward(work[0], work[1], left[0], row_twist)
    real, imag = middle(real, imag)
    real, imag = rows_inverse(real, imag, left[1], row_twist)
    work[0] = real
    work[1] = imag

    for start in range(0, side, CHUNK):
        rows = slice(start, start + CHUNK)
        store(rows, *lanes_inverse(work[0, rows, :], work[1, rows, :], right[1], lane_twist))


STRIP = 64
ROWS = 8


def numbers(groups, axis):
    return lax.broadcasted_iota(jnp.int32, (groups, ROWS, LANES), axis)


def bases(at, step):
    base = pl.multiple_of(at // step * step, step)
    return (base, at - base)


def cut(field, target, row, col, side):
    left, right = bases(col, LANES)
    top, under = bases(row, ROWS)
    groups = STRIP // ROWS
    take_rows = numbers(groups, 1) < ROWS - under
    take_cols = numbers(groups, 2) < LANES - right
    up, back = (lax.rem(ROWS - under, ROWS), lax.rem(LANES - right, LANES))

    def read(part, down, k):
        at = (part, pl.ds(pl.multiple_of(top + down, ROWS), STRIP + ROWS), pl.ds(pl.multiple_of(left + k * LANES, LANES), LANES))
        value = pltpu.roll(field[at], back, 1).reshape(groups + 1, ROWS, LANES)
        value = pltpu.roll(value, up, 1)
        return jnp.where(take_rows, value[:groups], value[1:])

    @pl.loop(0, side // STRIP)
    def _(step):
        down = pl.multiple_of(step * STRIP, STRIP)
        for part in range(field.shape[0]):
            turned = [read(part, down, k) for k in range(side // LANES + 1)]
            for k in range(side // LANES):
                value = jnp.where(take_cols, turned[k], turned[k + 1])
                target[part, pl.ds(down, STRIP), k * LANES : (k + 1) * LANES] = value.reshape(STRIP, LANES)


def place(field, source, row, col, side):
    left, right = bases(col, LANES)
    top, under = bases(row, ROWS)
    groups = STRIP // ROWS
    keep_rows = numbers(groups + 1, 1) >= under
    keep_cols = numbers(groups + 1, 2) >= right
    count = side // LANES
    edge = jnp.zeros((1, ROWS, LANES), jnp.float32)
    blank = jnp.zeros((groups + 1, ROWS, LANES), jnp.float32)

    def read(part, down, k):
        value = pltpu.roll(source[part, pl.ds(down, STRIP), k * LANES : (k + 1) * LANES], right, 1)
        value = pltpu.roll(value.reshape(groups, ROWS, LANES), under, 1)
        return jnp.where(
            keep_rows, jnp.concatenate([value, edge], axis=0), jnp.concatenate([edge, value], axis=0)
        )

    @pl.loop(0, side // STRIP)
    def _(step):
        down = pl.multiple_of(step * STRIP, STRIP)
        writes = []
        for part in range(field.shape[0]):
            turned = [blank] + [read(part, down, k) for k in range(count)] + [blank]
            for k in range(count + 1):
                value = jnp.where(keep_cols, turned[k + 1], turned[k]).reshape(STRIP + ROWS, LANES)
                spot = (
                    part,
                    pl.ds(pl.multiple_of(top + down, ROWS), STRIP + ROWS),
                    pl.ds(pl.multiple_of(left + k * LANES, LANES), LANES),
                )
                writes.append((spot, field[spot] + value))
        for spot, value in writes:
            field[spot] = value


def halo_spans(side, rows, cols):
    return [
        (0, cols, side, side),
        (side, cols, rows - side, side),
        (rows, 0, side, side),
        (rows, side, side, cols - side),
        (rows, cols, side, side),
    ]


def own_spans(side, rows, cols):
    rest_rows, rest_cols = (rows - side, cols - side)
    return [
        (0, 0, side, side),
        (0, side, side, rest_cols),
        (side, 0, rest_rows, side),
        (side, side, rest_rows, rest_cols),
    ]


def grad_spans(side, rows, cols):
    return own_spans(side, rows, cols) + [
        (0, cols, rows, side),
        (rows, side, side, cols - side),
        (rows, 0, side, side),
        (rows, cols, side, side),
    ]


def copies(blocks, field, spans, sem, outward):
    made = []
    for block, (row, col, rows, cols) in zip(blocks, spans):
        window = field.at[:, pl.ds(row, rows), pl.ds(col, cols)]
        source, target = (window, block) if outward else (block, window)
        made.append(pltpu.make_async_copy(source, target, sem.at[len(made)]))
    return made


def start_all(items):
    for item in items:
        item.start()


def wait_all(items):
    for item in items:
        item.wait()


def clear(field):
    rows = field.shape[1]

    @pl.loop(0, rows // 16)
    def _(step):
        at = pl.ds(pl.multiple_of(step * 16, 16), 16)
        for part in range(field.shape[0]):
            field[part, at, :] = jnp.zeros((16, field.shape[2]), jnp.float32)


def three_parts(value, axis):
    high = value.astype(jnp.bfloat16)
    rest = value - high.astype(jnp.float32)
    mid = rest.astype(jnp.bfloat16)
    low = (rest - mid.astype(jnp.float32)).astype(jnp.bfloat16)
    return jnp.concatenate([high, mid, low], axis=axis)


def even_odd(value):
    side = value.shape[0]
    first, second = (lax.broadcasted_iota(jnp.int32, (side, side), axis) for axis in (0, 1))

    def table(source, target):
        at = jnp.where(target < side // 2, 2 * target, 2 * target - side + 1)
        return jnp.where(source == at, 1.0, 0.0).astype(jnp.bfloat16)

    right, left = (table(first, second), table(second, first))
    value = dot(three_parts(value, 1), jnp.concatenate([right] * 3, axis=0))
    return dot(jnp.concatenate([left] * 3, axis=1), three_parts(value, 0))


def sort_kernel(side, slots, number, measured, angle, amplitude, phase):
    turned = even_odd(angle[...])
    phase[0] = jnp.cos(turned)
    phase[1] = jnp.sin(turned)

    @pl.loop(0, slots)
    def _(slot):
        amplitude[slot] = even_odd(measured[slot])


def sources(refs, spans, layer):
    if len(refs) < len(spans):
        tile = refs[0].at[:, layer]
        return ([tile, *refs[1:]], [(0, 0, *tile.shape[1:]), *spans[4:]])
    return (refs, spans)


def first_kernel(spans, side, slots, number, *refs):
    at, which, probe, phase, right, left, lane_twist, row_twist = refs[:8]
    patches, incoming, field, work, sem = refs[-5:]
    blocks, places = sources(refs[8:-5], spans, 0)
    moves = copies(blocks, field, places, sem, False)
    start_all(moves)
    wait_all(moves)

    @pl.loop(0, slots)
    def _(slot):
        @pl.when(which[slot] == number)
        def _():
            patch = patches.at[slot]
            out = incoming.at[slot]
            cut(field, patch, at[slot, 0], at[slot, 1], side)

            def load(rows):
                real, imag = (patch[0, rows, :], patch[1, rows, :])
                return (
                    probe[0, rows, :] * real - probe[1, rows, :] * imag,
                    probe[0, rows, :] * imag + probe[1, rows, :] * real,
                )

            def middle(real, imag):
                return (real * phase[0] - imag * phase[1], real * phase[1] + imag * phase[0])

            def store(rows, real, imag):
                out[0, rows, :] = real
                out[1, rows, :] = imag

            chain(load, middle, store, side, work, right, left, lane_twist, row_twist)


def second_kernel(spans, side, slots, number, *refs):
    at, which, probe, phase, patches, incoming_all, measured, right, left, lane_twist, row_twist = refs[:11]
    sums, *grads = refs[-18:-9]
    field, total1, total0, patch, delta, behind_all, work, sem, sem_out = refs[-9:]
    rows, cols = (total0.shape[1] - side, total0.shape[2] - side)
    places_out = grad_spans(side, rows, cols)
    blocks, places = sources(refs[11:-18], spans, 1)
    moves = copies(blocks, field, places, sem, False)
    start_all(moves)
    clear(total1)
    clear(total0)
    sums[...] = jnp.zeros_like(sums)
    wait_all(moves)

    @pl.loop(0, slots)
    def _(slot):
        @pl.when(which[slot] == number)
        def _():
            incoming = incoming_all.at[slot]
            out = behind_all.at[slot]
            cut(field, patch, at[slot, 0], at[slot, 1], side)

            def load(rows):
                real, imag = (patch[0, rows, :], patch[1, rows, :])
                in_real, in_imag = (incoming[0, rows, :], incoming[1, rows, :])
                return (real * in_real - imag * in_imag, real * in_imag + imag * in_real)

            def middle(real, imag):
                power = real * real + imag * imag
                factor = 1.0 - measured[slot] * lax.rsqrt(jnp.maximum(power, 0.01))
                return (real * factor, imag * factor)

            def store(rows, real, imag):
                in_real, in_imag = (incoming[0, rows, :], incoming[1, rows, :])
                delta[0, rows, :] = in_real * real + in_imag * imag
                delta[1, rows, :] = in_real * imag - in_imag * real
                own_real, own_imag = (patch[0, rows, :], patch[1, rows, :])
                out[0, rows, :] = own_real * real + own_imag * imag
                out[1, rows, :] = own_real * imag - own_imag * real

            chain(load, middle, store, side, work, right, left, lane_twist, row_twist)
            place(total1, delta, at[slot, 0], at[slot, 1], side)

    moves1 = copies([grad.at[1] for grad in grads], total1, places_out, sem, True)
    start_all(moves1)

    @pl.loop(0, slots)
    def _(slot):
        @pl.when(which[slot] == number)
        def _():
            behind = behind_all.at[slot]
            first = patches.at[slot]

            def load(rows):
                return (behind[0, rows, :], behind[1, rows, :])

            def middle(real, imag):
                return (real * phase[0] + imag * phase[1], imag * phase[0] - real * phase[1])

            def store(rows, real, imag):
                in_real, in_imag = (probe[0, rows, :], probe[1, rows, :])
                delta[0, rows, :] = in_real * real + in_imag * imag
                delta[1, rows, :] = in_real * imag - in_imag * real
                own_real, own_imag = (first[0, rows, :], first[1, rows, :])
                sums[0, rows, :] = sums[0, rows, :] + (own_real * real + own_imag * imag)
                sums[1, rows, :] = sums[1, rows, :] + (own_real * imag - own_imag * real)
                sums[2, rows, :] = sums[2, rows, :] + (own_real * own_real + own_imag * own_imag)

            chain(load, middle, store, side, work, right, left, lane_twist, row_twist)
            place(total0, delta, at[slot, 0], at[slot, 1], side)

    moves0 = copies([grad.at[0] for grad in grads], total0, places_out, sem_out, True)
    start_all(moves0)
    wait_all(moves1)
    wait_all(moves0)


VMEM = pltpu.MemorySpace.VMEM
SMEM = pltpu.MemorySpace.SMEM
ANY = pl.ANY


def spec(space):
    return pl.BlockSpec(memory_space=space)


def f32(*shape):
    return jax.ShapeDtypeStruct(shape, jnp.float32)


def quarters(field, side):
    return (
        field[:, :side, :side],
        field[:, :side, side:],
        field[:, side:, :side],
        field[:, side:, side:],
    )


def surroundings(own):
    low_left = shifted(own[0], "tile", -1)
    corner = shifted(low_left, "slab", -1)
    low_right = shifted(own[1], "tile", -1)
    top = shifted(own[0], "slab", -1)
    mid = shifted(own[2], "slab", -1)
    return [top, mid, low_left, low_right, corner]


def gathered(grads):
    low_right = shifted(grads[5], "tile", 1)
    corner = shifted(grads[7], "slab", 1)
    right = shifted(grads[4], "slab", 1)
    side = corner.shape[2]
    layers = []
    for layer in range(corner.shape[0]):
        low_left = shifted(grads[6][layer] + corner[layer], "tile", 1)
        layers.append(
            (
                grads[0][layer] + right[layer, :, :side] + low_left,
                grads[1][layer] + low_right[layer],
                grads[2][layer] + right[layer, :, side:],
                grads[3][layer],
            )
        )
    return layers


def stepped(layer, total, peak):
    new = [None] * len(layer)
    for block in (3, 1, 2, 0):
        new[block] = layer[block] - total[block] / peak
        peak, new[block] = lax.optimization_barrier((peak, new[block]))
    return tuple(new)


def doublings(axis):
    return [(axis, 1 << k) for k in range(lax.axis_size(axis).bit_length() - 1)]


def new_probe(sums, beam):
    tile = doublings("tile")
    cuts, rest = (doublings("slab") + tile[1:], tile[:1])
    value = sums
    mine = beam
    for axis, step in cuts:
        upper = (lax.axis_index(axis) & step) != 0
        half = value.shape[1] // 2
        first, last = (value[:, :half], value[:, half:])
        got = swapped(jnp.where(upper, first, last), axis, step)
        value = jnp.where(upper, last, first) + got
        mine = jnp.where(upper, mine[:, half:], mine[:, :half])
    for axis, step in rest:
        value = value + swapped(value, axis, step)
    mine = mine - value[:2] / (value[2] + 1.0)
    for axis, step in cuts[::-1]:
        upper = (lax.axis_index(axis) & step) != 0
        got = swapped(mine, axis, step)
        mine = jnp.concatenate([jnp.where(upper, got, mine), jnp.where(upper, mine, got)], axis=1)
    return mine


def update(object_field, probe, kernel_phase, measured, positions, batch):
    side = probe.shape[-1]
    tile_rows, tile_cols = object_field.shape[2:]
    slots = positions.shape[0]
    tables = dft_tables(side)
    spans = own_spans(side, tile_rows, tile_cols) + halo_spans(side, tile_rows, tile_cols)
    places_out = grad_spans(side, tile_rows, tile_cols)
    corner = jnp.stack([lax.axis_index("tile") * tile_rows, lax.axis_index("slab") * tile_cols])
    local_at = positions - corner[None, :]
    frames = f32(slots, 2, side, side)
    grad_shapes = [f32(2, 2, rows, cols) for _, _, rows, cols in places_out]
    whole = pltpu.VMEM((2, tile_rows + side, tile_cols + side), jnp.float32)
    plane = pltpu.VMEM((2, side, side), jnp.float32)
    sems = pltpu.SemaphoreType.DMA((len(spans),))
    smem2 = [spec(SMEM)] * 2
    out_sems = pltpu.SemaphoreType.DMA((len(places_out),))
    cost = pl.CostEstimate(flops=int(slots * 40e9), bytes_accessed=16 << 20, transcendentals=0)
    params = pltpu.CompilerParams(vmem_limit_bytes=48 << 20)

    def call(body, given, number, ins, outs, out_shapes, scratch):
        def run(*refs):
            body(*given, side, slots, number, *refs)

        return pl.pallas_call(
            run,
            in_specs=ins,
            out_specs=outs,
            out_shape=out_shapes,
            scratch_shapes=scratch,
            cost_estimate=cost,
            compiler_params=params,
        )

    amplitude, phase = call(
        sort_kernel, (), 0, [spec(VMEM)] * 2, [spec(VMEM)] * 2, [f32(slots, side, side), f32(2, side, side)], []
    )(measured, kernel_phase)
    layers = [quarters(object_field[:, layer], side) for layer in range(2)]
    beam = probe
    for number in range(BATCHES):
        around = [surroundings(layers[k]) for k in range(2)]
        owns = [[object_field] if number == 0 else list(layer) for layer in layers]
        fields = [own + halo for own, halo in zip(owns, around)]
        counts = [len(field) for field in fields]
        patches, incoming = call(
            first_kernel,
            (spans,),
            number,
            smem2 + [spec(VMEM)] * 6 + [spec(ANY)] * counts[0],
            [spec(VMEM)] * 2,
            [frames, frames],
            [whole, plane, sems],
        )(local_at, batch, beam, phase, *tables, *fields[0])
        sums, *grads = call(
            second_kernel,
            (spans,),
            number,
            smem2 + [spec(VMEM)] * 9 + [spec(ANY)] * counts[1],
            [spec(VMEM)] + [spec(ANY)] * len(grad_shapes),
            [f32(3, side, side)] + grad_shapes,
            [whole, whole, whole, plane, plane, pltpu.VMEM(frames.shape, jnp.float32), plane, sems, out_sems],
        )(local_at, batch, beam, phase, patches, incoming, amplitude, *tables, *fields[1])
        peak = jnp.max(beam[0] * beam[0] + beam[1] * beam[1])
        total = gathered(grads)
        layers = [stepped(layers[k], total[k], peak) for k in range(2)]
        beam = new_probe(sums, beam)
    result = jnp.zeros((2, 2 * tile_rows, tile_cols), jnp.float32)
    for block in (3, 1, 2, 0):
        for layer in (0, 1):
            row, col, _, _ = spans[block]
            result = lax.dynamic_update_slice(result, layers[layer][block], (0, layer * tile_rows + row, col))
    result = result.reshape(object_field.shape)
    return (result, beam)


def solution(mesh):
    in_specs = (
        P(None, None, "tile", "slab"),
        P(),
        P(),
        P(("tile", "slab"), None, None),
        P(("tile", "slab"), None),
        P(("tile", "slab")),
    )
    out_specs = (P(None, None, "tile", "slab"), P())
    return jax.shard_map(update, mesh=mesh, in_specs=in_specs, out_specs=out_specs, check_vma=False)
```
